32 devices in a mesh: dp: 1 (over z), ep: 32 (over y, x, core).
Axes of the slice: x: 4, y: 4, z: 1, core: 2. Of those that a mesh axis runs over, the one named last changes fastest.
The devices are a block of a 4x4x8 slice.
Arguments:
- x_tokens: bfloat16 [4096, 1536], P(('dp', 'ep'))
- slot_expert: int32 [320], replicated
- w1_slots: bfloat16 [320, 1536, 512], P('ep')
- w3_slots: bfloat16 [320, 1536, 512], P('ep')
- w2_slots: bfloat16 [320, 512, 1536], P('ep')
- assign: int32 [4096, 6], P(('dp', 'ep'))
- w_router: bfloat16 [1536, 64], replicated
- w1_shared: bfloat16 [1536, 1024], replicated
- w3_shared: bfloat16 [1536, 1024], replicated
- w2_shared: bfloat16 [1024, 1536], replicated
Outputs:
- output: bfloat16 [4096, 1536], P(('dp', 'ep'))
All inputs are finite; a program needn't handle non-finite values.
Results may differ from the reference program's by a relative error of at most 0.00101.
Values are sent between devices in bfloat16 or wider.
A program may use at most 768 MiB of HBM per device.

```python
import jax
import jax.numpy as jnp
from jax import lax

DIM_MODEL = 1536
FF_EXPERT = 512
FF_SHARED = 1024
NUM_EXPERTS = 64
TOP_K = 6
NUM_SLOTS = 320
GROUP_SIZE = 32
TOK_DEV = 128

TOKENS = TOK_DEV * GROUP_SIZE
CAP_ROWS = max(4, (3 * TOK_DEV * TOP_K) // NUM_SLOTS)
SEG_ROWS = min(TOKENS, GROUP_SIZE * CAP_ROWS)
ROUTE_SCALE = 2.5


def draw_routing(key_shared, key_part):
    key_rank, key_place = jax.random.split(key_shared, 2)
    rank_expert = jax.random.permutation(key_rank, NUM_EXPERTS).astype(jnp.int32)
    base_of_slot = jax.random.permutation(key_place, NUM_SLOTS).astype(jnp.int32)
    slot_expert = rank_expert[base_of_slot % NUM_EXPERTS]
    slot_of_base = jnp.argsort(base_of_slot).astype(jnp.int32)
    key_noise, key_coin, key_pick = jax.random.split(key_part, 3)
    rank_ids = jnp.arange(NUM_EXPERTS, dtype=jnp.int32)
    rank_bias = (2 * TOP_K * 4096) // (NUM_EXPERTS * (rank_ids + 1))
    noise_int = jax.random.randint(key_noise, (TOKENS, NUM_EXPERTS), 0, 4096, dtype=jnp.int32)
    token_ids = jnp.arange(TOKENS, dtype=jnp.int32)
    forced = token_ids < CAP_ROWS
    force_bonus = jnp.where(forced[:, None] & (rank_ids[None, :] == 0), 16384, 0)
    rank_score = (noise_int + rank_bias[None, :] + force_bonus) * NUM_EXPERTS + rank_ids[None, :]
    chosen_rank = lax.top_k(rank_score, TOP_K)[1].astype(jnp.int32)
    copies = (NUM_SLOTS - 1 - chosen_rank) // NUM_EXPERTS + 1
    coin_flip = jax.random.randint(key_coin, (TOKENS, TOP_K), 0, 2, dtype=jnp.int32)
    pick_copy = jax.random.randint(key_pick, (TOKENS, TOP_K), 0, 65536, dtype=jnp.int32) % copies
    keep_first = (coin_flip == 0) | (forced[:, None] & (chosen_rank == 0))
    copy_index = jnp.where(keep_first, 0, pick_copy)
    slot_pick = slot_of_base[chosen_rank + copy_index * NUM_EXPERTS]
    device_of = (token_ids // TOK_DEV)[:, None]
    group_key = (device_of * NUM_SLOTS + slot_pick).reshape(-1)
    sort_order = jnp.argsort(group_key, stable=True)
    sorted_key = group_key[sort_order]
    first_pos = jnp.searchsorted(sorted_key, sorted_key, side='left').astype(jnp.int32)
    rank_sorted = jnp.arange(TOKENS * TOP_K, dtype=jnp.int32) - first_pos
    rank_flat = jnp.zeros((TOKENS * TOP_K,), jnp.int32).at[sort_order].set(rank_sorted)
    assign = jnp.where(rank_flat < CAP_ROWS, slot_pick.reshape(-1), -1).reshape(TOKENS, TOP_K)
    return slot_expert, assign.astype(jnp.int32)


def setup_inputs(seed: int = 0, part: int = 0) -> dict:
    weight_keys = jax.random.split(jax.random.key(seed), 8)
    part_key = jax.random.fold_in(jax.random.key(seed + 1), part)
    key_tokens, key_route = jax.random.split(part_key, 2)
    slot_expert, assign = draw_routing(weight_keys[0], key_route)
    x_tokens = jax.random.normal(key_tokens, (TOKENS, DIM_MODEL), jnp.float32)
    w1_experts = jax.random.normal(weight_keys[1], (NUM_EXPERTS, DIM_MODEL, FF_EXPERT), jnp.float32) * DIM_MODEL ** -0.5
    w3_experts = jax.random.normal(weight_keys[2], (NUM_EXPERTS, DIM_MODEL, FF_EXPERT), jnp.float32) * DIM_MODEL ** -0.5
    w2_experts = jax.random.normal(weight_keys[3], (NUM_EXPERTS, FF_EXPERT, DIM_MODEL), jnp.float32) * FF_EXPERT ** -0.5
    w_router = jax.random.normal(weight_keys[4], (DIM_MODEL, NUM_EXPERTS), jnp.float32) * DIM_MODEL ** -0.5
    w1_shared = jax.random.normal(weight_keys[5], (DIM_MODEL, FF_SHARED), jnp.float32) * DIM_MODEL ** -0.5
    w3_shared = jax.random.normal(weight_keys[6], (DIM_MODEL, FF_SHARED), jnp.float32) * DIM_MODEL ** -0.5
    w2_shared = jax.random.normal(weight_keys[7], (FF_SHARED, DIM_MODEL), jnp.float32) * FF_SHARED ** -0.5
    return {
        'x_tokens': x_tokens.astype(jnp.bfloat16),
        'slot_expert': slot_expert,
        'w1_slots': w1_experts.astype(jnp.bfloat16)[slot_expert],
        'w3_slots': w3_experts.astype(jnp.bfloat16)[slot_expert],
        'w2_slots': w2_experts.astype(jnp.bfloat16)[slot_expert],
        'assign': assign,
        'w_router': w_router.astype(jnp.bfloat16),
        'w1_shared': w1_shared.astype(jnp.bfloat16),
        'w3_shared': w3_shared.astype(jnp.bfloat16),
        'w2_shared': w2_shared.astype(jnp.bfloat16),
    }


def gate_weights(x_tokens, assign, slot_expert, w_router):
    logits = jnp.dot(x_tokens, w_router, preferred_element_type=jnp.float32)
    gate_prob = jax.nn.sigmoid(logits)
    is_kept = assign >= 0
    chosen = slot_expert[jnp.maximum(assign, 0)]
    picked = jnp.where(is_kept, jnp.take_along_axis(gate_prob, chosen, axis=1), 0.0)
    gate_total = jnp.sum(picked, axis=1, keepdims=True)
    return ROUTE_SCALE * picked / jnp.maximum(gate_total, 1e-30), is_kept


def shared_expert(x_tokens, w1_shared, w3_shared, w2_shared):
    h_gate = jnp.dot(x_tokens, w1_shared, preferred_element_type=jnp.float32)
    h_up = jnp.dot(x_tokens, w3_shared, preferred_element_type=jnp.float32)
    mid_act = (jax.nn.silu(h_gate) * h_up).astype(jnp.bfloat16)
    return jnp.dot(mid_act, w2_shared, preferred_element_type=jnp.float32)


def reference(x_tokens, slot_expert, w1_slots, w3_slots, w2_slots, assign, w_router, w1_shared, w3_shared, w2_shared):
    route_weight, is_kept = gate_weights(x_tokens, assign, slot_expert, w_router)
    shared_out = shared_expert(x_tokens, w1_shared, w3_shared, w2_shared)
    flat_slot = jnp.where(is_kept, assign, NUM_SLOTS).reshape(-1)
    sort_order = jnp.argsort(flat_slot, stable=True)
    sorted_slot = flat_slot[sort_order]
    slot_ids = jnp.arange(NUM_SLOTS, dtype=jnp.int32)
    seg_start = jnp.searchsorted(sorted_slot, slot_ids, side='left').astype(jnp.int32)
    seg_end = jnp.searchsorted(sorted_slot, slot_ids, side='right').astype(jnp.int32)
    token_list = jnp.concatenate([(sort_order // TOP_K).astype(jnp.int32), jnp.zeros((SEG_ROWS,), jnp.int32)])
    weight_list = jnp.concatenate([route_weight.reshape(-1)[sort_order], jnp.zeros((SEG_ROWS,), route_weight.dtype)])
    row_offsets = jnp.arange(SEG_ROWS, dtype=jnp.int32)

    def slot_step(acc_rows, slot_id):
        seg_begin = seg_start[slot_id]
        row_ids = lax.dynamic_slice(token_list, (seg_begin,), (SEG_ROWS,))
        row_weight = lax.dynamic_slice(weight_list, (seg_begin,), (SEG_ROWS,))
        row_weight = jnp.where(row_offsets < seg_end[slot_id] - seg_begin, row_weight, 0.0)
        x_rows = x_tokens[row_ids]
        h_gate = jnp.dot(x_rows, w1_slots[slot_id], preferred_element_type=jnp.float32)
        h_up = jnp.dot(x_rows, w3_slots[slot_id], preferred_element_type=jnp.float32)
        mid_act = (jax.nn.silu(h_gate) * h_up).astype(jnp.bfloat16)
        out_rows = jnp.dot(mid_act, w2_slots[slot_id], preferred_element_type=jnp.float32).astype(jnp.bfloat16)
        acc_rows = acc_rows.at[row_ids].add(row_weight[:, None] * out_rows.astype(jnp.float32))
        return acc_rows, None

    routed = lax.scan(slot_step, jnp.zeros((TOKENS, DIM_MODEL), jnp.float32), slot_ids)[0]
    return (shared_out + routed).astype(jnp.bfloat16)
```

```python
import functools
import math

import jax
import jax.numpy as jnp
import numpy as np
from jax import lax
from jax.experimental import pallas as pl
from jax.experimental.pallas import tpu as pltpu
from jax.sharding import PartitionSpec as P

ROUTE_SCALE = 2.5
LANES = 128
BLOCK_ROWS = (128, 48, 16, 16, 16)
AIM_ROWS = (112, 44, 14, 11, 11)
SLOT_ROWS = 176
WEIGHT_BUFFERS = 7
BALANCE_STEPS = 3
BF16, F32 = jnp.bfloat16, jnp.float32


def gate_weights(x_tokens, assign, slot_expert, w_router):
    logits = jnp.dot(x_tokens, w_router, preferred_element_type=jnp.float32)
    gate_prob = jax.nn.sigmoid(logits)
    is_kept = assign >= 0
    chosen = jnp.take(slot_expert, jnp.maximum(assign, 0))
    picked = jnp.where(is_kept, jnp.take_along_axis(gate_prob, chosen, axis=1), 0.0)
    gate_total = jnp.sum(picked, axis=1, keepdims=True)
    return ROUTE_SCALE * picked / jnp.maximum(gate_total, 1e-30), is_kept


def shared_expert(x_tokens, w1_shared, w3_shared, w2_shared):
    h_gate = jnp.dot(x_tokens, w1_shared, preferred_element_type=jnp.float32)
    h_up = jnp.dot(x_tokens, w3_shared, preferred_element_type=jnp.float32)
    mid_act = (jax.nn.silu(h_gate) * h_up).astype(jnp.bfloat16)
    return jnp.dot(mid_act, w2_shared, preferred_element_type=jnp.float32)


def padded_step(group_size, x_tokens, slot_expert, w1_slots, w3_slots, w2_slots, assign, w_router, shared_out):
    tok_dev, dim_model = x_tokens.shape
    top_k = assign.shape[1]
    local_slots = w1_slots.shape[0]
    num_slots = local_slots * group_size
    cap_rows = max(4, (3 * tok_dev * top_k) // num_slots)
    route_weight, is_kept = gate_weights(x_tokens, assign, slot_expert, w_router)
    flat_slot = jnp.where(is_kept, assign, num_slots).reshape(-1)
    onehot = (flat_slot[:, None] == jnp.arange(num_slots, dtype=jnp.int32)[None, :]).astype(jnp.int32)
    slot_rank = jnp.sum(jnp.cumsum(onehot, axis=0) * onehot, axis=1) - 1
    dummy_row = num_slots * cap_rows
    row_pos = jnp.where(flat_slot < num_slots, flat_slot * cap_rows + slot_rank, dummy_row)
    token_ids = jnp.arange(tok_dev * top_k, dtype=jnp.int32) // top_k
    row_token = jnp.full((dummy_row + 1,), tok_dev, jnp.int32).at[row_pos].set(token_ids)[:dummy_row]
    send_rows = jnp.take(x_tokens, row_token, axis=0, mode='fill', fill_value=0)
    recv_rows = lax.all_to_all(send_rows, 'ep', 0, 0, tiled=True)
    recv_rows = recv_rows.reshape(group_size, local_slots, cap_rows, dim_model)
    h_gate = jnp.einsum('jlcd,ldf->jlcf', recv_rows, w1_slots, preferred_element_type=jnp.float32)
    h_up = jnp.einsum('jlcd,ldf->jlcf', recv_rows, w3_slots, preferred_element_type=jnp.float32)
    mid_act = (jax.nn.silu(h_gate) * h_up).astype(jnp.bfloat16)
    expert_out = jnp.einsum('jlcf,lfd->jlcd', mid_act, w2_slots, preferred_element_type=jnp.float32).astype(jnp.bfloat16)
    back_rows = lax.all_to_all(expert_out.reshape(dummy_row, dim_model), 'ep', 0, 0, tiled=True)
    gathered = jnp.take(back_rows, jnp.minimum(row_pos, dummy_row - 1), axis=0).reshape(tok_dev, top_k, dim_model)
    routed = jnp.sum(route_weight[:, :, None] * gathered, axis=1)
    return (shared_out + routed).astype(jnp.bfloat16)


class Plan:
    def __init__(self, group_size):
        self.group_size = group_size
        self.side = math.isqrt(group_size // 2)
        assert 2 * self.side * self.side == group_size
        side = self.side
        ring = lambda d: min(d % side, -d % side)
        peers = [(dy, dx, dc) for dy in range(side) for dx in range(side) for dc in range(2)]
        dist = {p: min(ring(p[0]) + ring(p[1]), len(BLOCK_ROWS) - 1) for p in peers}
        self.rows = {p: BLOCK_ROWS[dist[p]] for p in peers}
        self.aim = {p: AIM_ROWS[dist[p]] for p in peers}
        order = sorted((p for p in peers if p != (0, 0, 0)), key=lambda p: (-self.rows[p], dist[p], p))
        far = [p for p in order if dist[p] > 1]
        far = sorted(far, key=lambda p: (-dist[p], p[2], p))
        near = [p for p in order if dist[p] == 1]
        chunks = []
        while near or far:
            chunk, room = [], LANES
            while near and room >= self.rows[near[0]]:
                chunk.append(near.pop(0))
                room -= self.rows[chunk[-1]]
            while far and room >= self.rows[far[0]]:
                chunk.append(far.pop(0))
                room -= self.rows[chunk[-1]]
            chunks.append(chunk)
        chunks += [[p] for p in order if dist[p] == 0] + [[(0, 0, 0)]]
        self.chunks = chunks
        self.start, self.holes = {}, []
        for index, chunk in enumerate(chunks):
            at = index * LANES
            for p in chunk:
                self.start[p] = at
                at += self.rows[p]
            if at < (index + 1) * LANES:
                self.holes.append((at, (index + 1) * LANES - at))
        self.total = len(chunks) * LANES
        self.peers = [p for chunk in chunks for p in chunk if p != (0, 0, 0)]

    def relative(self, me, p, sign):
        side = self.side
        chip = me // 2
        y = (chip // side + sign * p[0] + side) % side
        x = (chip % side + sign * p[1] + side) % side
        return (y * side + x) * 2 + (me + p[2]) % 2

    def table(self, local_slots, width):
        out = np.zeros((self.group_size, 3, width), np.float32)
        out[:, :2] = 1.0
        for me in range(self.group_size):
            for p in self.rows:
                dev = self.relative(me, p, 1)
                cols = slice(dev * local_slots, (dev + 1) * local_slots)
                out[me, 0, cols] = self.aim[p]
                out[me, 1, cols] = self.rows[p]
                out[me, 2, cols] = self.start[p]
        return out.reshape(self.group_size, 3 * width)


def dot(a, b, dims=((1,), (0,))):
    return lax.dot_general(a, b, (dims, ((), ())), preferred_element_type=F32)


def route_kernel(plan, local_slots, width, x_ref, a_ref, ecol_ref, erow_ref, wr_ref, tab_ref, send_ref, meta_ref, wc_ref):
    me = lax.axis_index('ep')
    tok, top_k = a_ref.shape
    num_experts = wr_ref.shape[1]
    iota = lambda shape, d: lax.broadcasted_iota(jnp.int32, shape, d)
    fiota = lambda shape, d: iota(shape, d).astype(F32)
    aim = tab_ref[pl.ds(me, 1), pl.ds(0, width)]
    room = tab_ref[pl.ds(me, 1), pl.ds(width, width)]
    base = tab_ref[pl.ds(me, 1), pl.ds(2 * width, width)]
    x = x_ref[...]
    gate = jax.nn.sigmoid(dot(x, wr_ref[...]))
    ecol, erow = ecol_ref[...], erow_ref[...]
    expert_of = (ecol == iota((width, num_experts), 1)).astype(F32).astype(BF16)
    below = (iota((tok, tok), 0) > iota((tok, tok), 1)).astype(F32).astype(BF16)
    carry = jnp.zeros((1, num_experts), F32)
    slots = iota((tok, width), 1)
    hot, rank, picked = [], [], []
    gate_total = jnp.zeros((tok, 1), F32)
    for k in range(top_k):
        onehot = (a_ref[:, k:k + 1] == slots).astype(F32).astype(BF16)
        b = dot(onehot, expert_of)
        bb = b.astype(BF16)
        picked.append(jnp.sum(b * gate, axis=1, keepdims=True))
        gate_total = gate_total + picked[-1]
        before = dot(below, bb) + carry
        rank.append(jnp.sum(b * before, axis=1, keepdims=True))
        carry = carry + jnp.sum(b, axis=0, keepdims=True)
        hot.append(bb)
    wide = lambda row: jnp.broadcast_to(row, (8, row.shape[1]))
    count = dot(wide(carry).astype(BF16), expert_of, ((1,), (1,)))
    row_id, col_id = iota((width, width), 0), iota((width, width), 1)
    dev_of = lambda i: jnp.floor((i.astype(F32) + 0.5) / local_slots)
    mask = lambda m: m.astype(F32).astype(BF16)
    same = ecol == erow
    near = dev_of(row_id) == dev_of(col_id)
    same_m, near_m = mask(same), mask(near)
    aim8, room8, base8 = wide(aim), wide(room), wide(base)
    v = aim8
    for _ in range(BALANCE_STEPS):
        total = dot(v.astype(BF16), same_m)
        load = dot((count * v / total).astype(BF16), near_m)
        v = v * aim8 / jnp.maximum(load, 0.01)
        v = v / dot(v.astype(BF16), same_m)
    share = jnp.clip(jnp.floor(v * 192.0 + 0.5), 1.0, 200.0).astype(BF16)
    total = dot(share, same_m)
    upto = dot(share, mask(same & (row_id <= col_id)))
    ahead = dot(share, mask(same & (row_id < col_id)))
    end = jnp.floor(count * (upto / total) + 0.5)
    begin = jnp.floor(count * (ahead / total) + 0.5)
    take = end - begin
    take_m = take.astype(BF16)
    load = dot(take_m, near_m)
    first = base8 + dot(take_m, mask(near & (row_id < col_id)))
    full = jnp.max(jnp.where(load > room8, 1.0, 0.0))
    down = lambda row: jnp.broadcast_to(row[0:1], (LANES, width)).T
    first_d, last_d = down(first), down(first + take)
    s_col = iota((width, LANES), 0)
    local_d = s_col.astype(F32) - local_slots * dev_of(s_col) + 1.0
    lane = fiota((width, LANES), 1)
    for c in range(plan.total // LANES):
        r = lane + float(c * LANES)
        inside = (r >= first_d) & (r < last_d)
        line = jnp.sum(jnp.where(inside, local_d, 0.0), axis=0, keepdims=True)
        meta_ref[c:c + 1, :] = jnp.where(full > 0.5, 1024.0, line)
    wc = jnp.zeros((tok, plan.total), F32)
    rows = fiota((tok, plan.total), 1)
    places = jnp.zeros((tok, LANES), F32)
    lane_t = iota((tok, LANES), 1)
    for k in range(top_k):
        mine = dot(hot[k], expert_of, ((1,), (1,))) > 0.5
        mine = mine & (rank[k] >= begin[0:1]) & (rank[k] < end[0:1])
        place = jnp.sum(jnp.where(mine, first[0:1] - begin[0:1] + (rank[k] + 1.0), 0.0), axis=1, keepdims=True) - 1.0
        weight = ROUTE_SCALE * picked[k] / jnp.maximum(gate_total, 1e-30)
        wc = wc + jnp.where(rows == place, weight, 0.0)
        places = jnp.where(lane_t == k, place, places)
    wc_ref[...] = wc
    places = places.T
    at = fiota((plan.total, tok), 0)
    pick = jnp.zeros((plan.total, tok), F32)
    for k in range(top_k):
        pick = pick + jnp.where(at == places[k:k + 1, :], 1.0, 0.0)
    pick = pick.astype(BF16)
    half = x.shape[1] // 2
    for h in range(2):
        send_ref[:, h * half:(h + 1) * half] = dot(pick, x[:, h * half:(h + 1) * half]).astype(BF16)


def exchange_kernel(plan, send, meta, wc, z, w1, w3, w2, y, flag, recv, outb, back, xo, metas, flags, mine,
                    w1b, w3b, w2b, f_row, f_col, s_send, s_recv, m_send, m_recv, b_send, b_recv, g_send, g_recv, wsem):
    me = lax.axis_index('ep')
    n_slots = w1.shape[0]
    n_buf = w1b.shape[0]
    n_peer = len(plan.peers)
    n_chunk = plan.total // LANES
    total = n_slots * SLOT_ROWS
    iota = lambda shape, d: lax.broadcasted_iota(jnp.int32, shape, d)
    dst = [plan.relative(me, p, 1) for p in plan.peers]
    src = [plan.relative(me, p, -1) for p in plan.peers]

    def weight_copies(slot, buf):
        return [pltpu.make_async_copy(w.at[slot], wb.at[buf], wsem.at[i, buf])
                for i, (w, wb) in enumerate(((w1, w1b), (w3, w3b), (w2, w2b)))]

    for slot in range(min(n_buf, n_slots)):
        for copy in weight_copies(slot, slot):
            copy.start()
    barrier = pltpu.get_barrier_semaphore()
    for d in dst:
        pl.semaphore_signal(barrier, inc=1, device_id={'ep': d}, device_id_type=pl.DeviceIdType.MESH)
    for at, rows in plan.holes:
        recv[pl.ds(at, rows), :] = jnp.zeros((rows, recv.shape[1]), BF16)
        back[pl.ds(at, rows), :] = jnp.zeros((rows, back.shape[1]), BF16)
    pl.semaphore_wait(barrier, n_peer)

    def remote(a, b, s0, s1, d):
        return pltpu.make_async_remote_copy(src_ref=a, dst_ref=b, send_sem=s0, recv_sem=s1,
                                            device_id={'ep': d}, device_id_type=pl.DeviceIdType.MESH)

    block = lambda p: pl.ds(plan.start[p], plan.rows[p])
    meta_cp = [remote(meta, metas.at[i], m_send.at[i], m_recv.at[i], dst[i]) for i in range(n_peer)]
    row_cp = [remote(send.at[block(p)], recv.at[block(p)], s_send.at[i], s_recv.at[i], dst[i])
              for i, p in enumerate(plan.peers)]
    for copy in meta_cp:
        copy.start()
    for copy in row_cp:
        copy.start()
    own = block((0, 0, 0))
    recv[own, :] = send[own, :]

    cell = iota((n_chunk, LANES), 0) * LANES + iota((n_chunk, LANES), 1)
    inside = lambda p: (cell >= plan.start[p]) & (cell < plan.start[p] + plan.rows[p])
    got = jnp.where(inside((0, 0, 0)), meta[...], 0.0)
    for i, p in enumerate(plan.peers):
        meta_cp[i].wait_recv()
        got = got + jnp.where(inside(p), metas[i], 0.0)
    tri = (iota((LANES, LANES), 0) <= iota((LANES, LANES), 1)).astype(F32).astype(BF16)
    prev = (iota((n_chunk, n_chunk), 0) > iota((n_chunk, n_chunk), 1)).astype(F32).astype(BF16)
    flat = jnp.full((n_chunk, LANES), -1.0, F32)
    bad = jnp.max(got) > 512.0
    worst = jnp.zeros((n_chunk, LANES), F32)
    for slot in range(n_slots):
        hit = got == float(slot + 1)
        hit_m = hit.astype(F32).astype(BF16)
        rank = dot(hit_m, tri) - 1.0 + jnp.sum(dot(prev, hit_m), axis=1, keepdims=True)
        flat = jnp.where(hit & (rank < float(SLOT_ROWS)), rank + float(slot * SLOT_ROWS), flat)
        worst = jnp.maximum(worst, jnp.where(hit, rank, 0.0))
    bad = jnp.where(bad | (jnp.max(worst) > SLOT_ROWS - 0.5), 1.0, 0.0)
    mine[...] = jnp.full(mine.shape, bad, F32)
    f_row[...] = flat
    f_col[...] = jnp.concatenate([flat, jnp.zeros((LANES - n_chunk, LANES), F32)], axis=0).T

    for copy in row_cp:
        copy.wait_recv()

    def one_slot(slot, _):
        buf = lax.rem(slot, n_buf)
        want = (iota((SLOT_ROWS, LANES), 0) + slot * SLOT_ROWS).astype(F32)
        pick = jnp.concatenate([jnp.where(want == f_row[c:c + 1, :], 1.0, 0.0).astype(BF16)
                                for c in range(n_chunk)], axis=1)
        x = dot(pick, recv[...]).astype(BF16)
        for copy in weight_copies(slot, buf):
            copy.wait()
        h = dot(x, w1b[buf])
        h = (h * jax.nn.sigmoid(h)) * dot(x, w3b[buf])
        o = dot(h.astype(BF16), w2b[buf])
        xo[pl.ds(pl.multiple_of(slot * SLOT_ROWS, 16), SLOT_ROWS), :] = o.astype(BF16)

        @pl.when(slot + n_buf < n_slots)
        def _():
            for copy in weight_copies(slot + n_buf, buf):
                copy.start()
        return 0

    lax.fori_loop(0, n_slots, one_slot, 0)

    flag_cp = [remote(mine, flags.at[i], g_send.at[i], g_recv.at[i], src[i]) for i in range(n_peer)]
    back_cp = [remote(outb.at[block(p)], back.at[block(p)], b_send.at[i], b_recv.at[i], src[i])
               for i, p in enumerate(plan.peers)]
    for copy in flag_cp:
        copy.start()
    lane = iota((LANES, total), 1).astype(F32)

    def scatter(c):
        pick = jnp.where(lane == f_col[:, c:c + 1], 1.0, 0.0).astype(BF16)
        return dot(pick, xo[...]).astype(BF16)

    for c, chunk in enumerate(plan.chunks):
        if chunk == [(0, 0, 0)]:
            back[pl.ds(c * LANES, LANES), :] = scatter(c)
        else:
            outb[pl.ds(c * LANES, LANES), :] = scatter(c)
        if c:
            for i, p in enumerate(plan.peers):
                if p in plan.chunks[c - 1]:
                    back_cp[i].start()
    any_bad = jnp.full(mine.shape, bad, F32)
    for i in range(n_peer):
        flag_cp[i].wait_recv()
        any_bad = jnp.maximum(any_bad, flags[i])
    flag[...] = any_bad
    w = wc[...]
    w_hi = w.astype(BF16)
    rest = w - w_hi.astype(F32)
    w_mid = rest.astype(BF16)
    w_lo = (rest - w_mid.astype(F32)).astype(BF16)
    for copy in back_cp:
        copy.wait_recv()
    half = y.shape[1] // 2
    for h in range(2):
        cols = slice(h * half, (h + 1) * half)
        b = back[:, cols]
        y[:, cols] = (z[:, cols] + (dot(w_hi, b) + (dot(w_mid, b) + dot(w_lo, b)))).astype(y.dtype)
    for group in (meta_cp, row_cp, flag_cp, back_cp):
        for copy in group:
            copy.wait_send()


def solution(mesh):
    group_size = mesh.shape['ep']
    plan = Plan(group_size)

    def device_step(x_tokens, slot_expert, w1_slots, w3_slots, w2_slots, assign, w_router, w1_shared, w3_shared, w2_shared):
        tok_dev, dim_model = x_tokens.shape
        local_slots, _, dim_ff = w1_slots.shape
        num_slots = local_slots * group_size
        width = -(-num_slots // LANES) * LANES
        n_chunk = plan.total // LANES
        experts = jnp.pad(slot_expert, (0, width - num_slots), constant_values=-1)
        vmem = pl.BlockSpec(memory_space=pltpu.VMEM)
        hbm = pl.BlockSpec(memory_space=pl.ANY)
        send, meta, wc = pl.pallas_call(
            functools.partial(route_kernel, plan, local_slots, width),
            out_shape=(jax.ShapeDtypeStruct((plan.total, dim_model), BF16),
                       jax.ShapeDtypeStruct((n_chunk, LANES), F32),
                       jax.ShapeDtypeStruct((tok_dev, plan.total), F32)),
            in_specs=[vmem] * 6,
            out_specs=(vmem, vmem, vmem),
            compiler_params=pltpu.CompilerParams(vmem_limit_bytes=40 * 2**20),
            name='route',
        )(x_tokens, assign, experts.reshape(width, 1), experts.reshape(1, width), w_router,
          jnp.asarray(plan.table(local_slots, width)))
        shared_out = shared_expert(x_tokens, w1_shared, w3_shared, w2_shared)
        n_peer = len(plan.peers)
        n_buf = min(WEIGHT_BUFFERS, local_slots)
        dma = pltpu.SemaphoreType.DMA
        y, flag = pl.pallas_call(
            functools.partial(exchange_kernel, plan),
            out_shape=(jax.ShapeDtypeStruct((tok_dev, dim_model), BF16),
                       jax.ShapeDtypeStruct((8, LANES), F32)),
            in_specs=[vmem] * 4 + [hbm] * 3,
            out_specs=(vmem, vmem),
            scratch_shapes=[
                pltpu.VMEM((plan.total, dim_model), BF16),
                pltpu.VMEM((plan.total, dim_model), BF16),
                pltpu.VMEM((plan.total, dim_model), BF16),
                pltpu.VMEM((local_slots * SLOT_ROWS, dim_model), BF16),
                pltpu.VMEM((n_peer, n_chunk, LANES), F32),
                pltpu.VMEM((n_peer, 8, LANES), F32),
                pltpu.VMEM((8, LANES), F32),
                pltpu.VMEM((n_buf, dim_model, dim_ff), BF16),
                pltpu.VMEM((n_buf, dim_model, dim_ff), BF16),
                pltpu.VMEM((n_buf, dim_ff, dim_model), BF16),
                pltpu.VMEM((n_chunk, LANES), F32),
                pltpu.VMEM((LANES, LANES), F32),
            ] + [dma((n_peer,))] * 8 + [dma((3, n_buf))],
            compiler_params=pltpu.CompilerParams(
                collective_id=0, has_side_effects=True, vmem_limit_bytes=67_000_000),
            name='exchange',
        )(send, meta, wc, shared_out, w1_slots, w3_slots, w2_slots)
        return lax.cond(
            flag[0, 0] > 0.5,
            lambda: padded_step(group_size, x_tokens, slot_expert, w1_slots, w3_slots, w2_slots, assign, w_router, shared_out),
            lambda: y)

    token_spec = P(('dp', 'ep'), None)
    slot_spec = P('ep', None, None)
    return jax.shard_map(device_step, mesh=mesh, in_specs=(token_spec, P(), slot_spec, slot_spec, slot_spec, token_spec, P(), P(), P(), P()), out_specs=token_spec, check_vma=False)
```
